256 devices in a mesh: section: 4 (over y), fsdp: 64 (over z, x, core).
Axes of the slice: x: 4, y: 4, z: 8, core: 2. Of those that a mesh axis runs over, the one named last changes fastest.
Arguments:
- residual_input: bfloat16 [2, 4096, 8192], P(None, 'fsdp'), may hold values from -16 to 16
- output_gradient: bfloat16 [2, 4096, 8192], P(None, 'fsdp'), may hold values from -0.0068359375 to 0.0068359375
- value_projection_weight: bfloat16 [4, 8192, 512], P('section', 'fsdp'), may hold values from -0.0625 to 0.0625
- output_weight: bfloat16 [4, 512, 8192], P('section', None, 'fsdp'), may hold values from -0.25 to 0.25
- adapter_down_weight: bfloat16 [4, 8192, 160], P('section'), may hold values from -0.0625 to 0.0625
- adapter_up_weight: bfloat16 [4, 160, 512], P('section'), may hold values from -0.625 to 0.625
- input_norm_scale: float32 [4, 8192], P('section'), may hold values from 0.25 to 1.75
- segment_adapter_index: int32 [2, 128], P(None, 'fsdp'), may hold values from 0 to 3
- adapter_rank_blocks: int32 [4], replicated, may hold values from 1 to 16, 20 in all
Outputs:
- grad_down: float32 [4, 8192, 160], P('section', 'fsdp')
- grad_up: float32 [4, 160, 512], P('section', None, 'fsdp')
The draws below stay inside these ranges and needn't reach their ends.
Inputs may be any that keep to these rules, and one draw needn't show every extreme that they name: `segment_adapter_index`: adapter of each block of 32 consecutive tokens. `adapter_rank_blocks`: the entries sum to 20.
All inputs are finite; a program needn't handle non-finite values.
Results may differ from the reference program's by a relative error of at most 0.014.
Values may be sent and summed in bfloat16 or wider, within the bound.
No kernel may reach another device: no remote copies, remote signals or barrier semaphores. Data moves between devices by JAX's collectives and lax.ppermute only.
A program may use at most 128 MiB of HBM per device.

```python
import math
import jax
import jax.numpy as jnp
import numpy as np
from jax import lax

MODEL_WIDTH = 8192
VALUE_WIDTH = 512
ADAPTERS = 4
RMAX = 128
RBLOCKS = 20
SEG = 32
M = 2
LAYER_SECTIONS = 4
TOKENS = 4096
PACKED_COLUMNS = 160


def set_ends(result, stream_key, smallest, largest):
    extent = result.shape
    spot = [jax.random.randint(jax.random.fold_in(stream_key, axis), (), 0, extent[axis]) for axis in range(len(extent))]
    result = result.at[tuple(spot)].set(smallest)
    longest = extent.index(max(extent))
    spot[longest] = (spot[longest] + 1) % extent[longest]
    return result.at[tuple(spot)].set(largest)


def spiked(array, rng, source, target, blocks, factor):
    owner, partner = [(jnp.arange(array.shape[position]) // (array.shape[position] // blocks)).reshape([-1 if axis == position else 1 for axis in range(array.ndim)]) for position in (source, target)]
    chosen = jax.random.permutation(rng, blocks)[partner]
    strong = (owner == chosen) | (owner == (partner + blocks // 2) % blocks)
    return jnp.where(strong, factor * array, array)


def block_scale(key, extent, split, low, top_value):
    def one(axis_at, shards_of):
        draws = jax.random.uniform(jax.random.fold_in(jax.random.fold_in(key, 6), axis_at), (shards_of,), jnp.float32, low / len(split), top_value / len(split))
        return jnp.repeat(jnp.exp(draws), extent[axis_at] // shards_of).reshape((-1,) + (1,) * (len(extent) - axis_at - 1))

    factor_of = one(*split[0])
    for cut in split[1:]:
        factor_of = factor_of * one(*cut)
    return factor_of


def length_profile(count, total, bound, lean):
    portions = [(1 << 20) // math.isqrt(standing ** lean) + 1 for standing in range(2, count + 1)]
    rest, given = total - bound - (count - 1), [1] * (count - 1)
    while rest > 0:
        candidates = [i for i in range(count - 1) if given[i] < bound]
        mass, budget = sum([portions[i] for i in candidates]), rest
        for i in candidates:
            addition = min(bound - given[i], max(1, budget * portions[i] // mass), rest)
            given[i] = given[i] + addition
            rest = rest - addition
    return np.array([bound] + given)


def uneven(own_key, number_of, total, limit, slope):
    if number_of == 2:
        one = jax.random.randint(own_key, (), max(1, total - limit), min(limit, total - 1) + 1)
        return jnp.stack([one, total - one])
    sizes = jnp.asarray(length_profile(number_of, total, limit, slope), jnp.int32)
    couples = (number_of - 1) // 2
    source_of, taker = sizes[1:1 + 2 * couples:2], sizes[2:2 + 2 * couples:2]
    margin = jnp.minimum(source_of - 1, limit - taker)
    moved = jax.random.randint(jax.random.fold_in(own_key, 1), (couples,), 0, 1 << 20) % (margin + 1)
    sizes = sizes.at[1:1 + 2 * couples:2].set(source_of - moved).at[2:2 + 2 * couples:2].set(taker + moved)
    return sizes[jax.random.permutation(jax.random.fold_in(own_key, 2), number_of)]


def noise(stream_key, shape, scale, bound, pieces=(), kind=jnp.bfloat16):
    values = jax.random.normal(stream_key, shape, jnp.float32) * scale
    if len(pieces) > 0:
        values = block_scale(stream_key, shape, pieces, -0.22, 0.18) * values
    return jnp.clip(values, min=-bound, max=bound).astype(kind)


def bell_draw_with(stream_key, dims, spread, bound, split, heavy, held_as=jnp.bfloat16):
    array = spread * jax.random.normal(stream_key, dims, jnp.float32)
    if split:
        array = array * block_scale(stream_key, dims, split, -0.22, 0.18)
    return jnp.clip(spiked(array, jax.random.fold_in(stream_key, 3), *heavy), -bound, bound).astype(held_as)


def setup_inputs(seed: int = 0) -> dict:
    keys = jax.random.split(jax.random.key(seed), 10)
    residual_input = bell_draw_with(keys[0], (M, TOKENS, MODEL_WIDTH), 1.0, 16.0, ((1, 64),), (1, 2, 64, 4.0))
    output_gradient = noise(keys[1], (M, TOKENS, MODEL_WIDTH), (0.1 / (M * TOKENS) ** 0.5), 0.0068359375, ((1, 64),))
    value_projection_weight = noise(keys[2], (LAYER_SECTIONS, MODEL_WIDTH, VALUE_WIDTH), MODEL_WIDTH ** -0.5, 0.0625, ((0, 4), (1, 64)))
    output_weight = noise(keys[3], (LAYER_SECTIONS, VALUE_WIDTH, MODEL_WIDTH), VALUE_WIDTH ** -0.5, 0.25, ((0, 4), (2, 64)))
    adapter_down_weight = noise(keys[4], (LAYER_SECTIONS, MODEL_WIDTH, PACKED_COLUMNS), MODEL_WIDTH ** -0.5, 0.0625, ((0, 4),))
    adapter_up_weight = noise(keys[5], (LAYER_SECTIONS, PACKED_COLUMNS, VALUE_WIDTH), 0.1, 0.625, ((0, 4),))
    input_norm_scale = jnp.clip(1.0 + 0.15 * jax.random.normal(keys[6], (LAYER_SECTIONS, MODEL_WIDTH), jnp.float32), 0.25, 1.75)
    segment_adapter_index = set_ends(jax.random.randint(keys[7], (M, TOKENS // SEG), 0, ADAPTERS), jax.random.fold_in(keys[7], 1), 0, ADAPTERS - 1).astype(jnp.int32)
    adapter_rank_blocks = uneven(keys[8], ADAPTERS, RBLOCKS, RMAX // 8, 2).astype(jnp.int32)
    return {"residual_input": residual_input, "output_gradient": output_gradient, "value_projection_weight": value_projection_weight, "output_weight": output_weight, "adapter_down_weight": adapter_down_weight, "adapter_up_weight": adapter_up_weight, "input_norm_scale": input_norm_scale, "segment_adapter_index": segment_adapter_index, "adapter_rank_blocks": adapter_rank_blocks}


EPSILON = 1e-06
ADAPTER_ALPHA = 32.0

def coefficients(segments, adapter_rank_blocks):
    rank_sizes = 8 * adapter_rank_blocks
    rank_ends = jnp.cumsum(rank_sizes).astype(jnp.int32)
    columns = jnp.arange(PACKED_COLUMNS, dtype=jnp.int32)
    column_owner = lax.optimization_barrier(jnp.sum((columns[:, None] >= rank_ends[None, :]).astype(jnp.int32), axis=1))
    token_adapter = jnp.repeat(segments, SEG)
    selector = (token_adapter[:, None] == jnp.arange(ADAPTERS, dtype=jnp.int32)[None, :]).astype(jnp.float32)
    token_rank_mask = lax.optimization_barrier(jnp.sum(selector * rank_sizes.astype(jnp.float32)[None, :], axis=1))
    adapter_matches = (token_adapter[:, None] == column_owner[None, :]).astype(jnp.float32)
    return adapter_matches * (ADAPTER_ALPHA / token_rank_mask)[:, None]

def section_forward_pass(layer_activation, norm_gains, value_weight, out_weight, down_matrix, up_matrix, scale_coefficient):
    widened = layer_activation.astype(jnp.float32)
    inverse_root_mean = lax.rsqrt(lax.optimization_barrier(jnp.mean(widened * widened, axis=-1)) + EPSILON)
    normalized_input = (widened * inverse_root_mean[:, None] * norm_gains[None, :]).astype(jnp.bfloat16)
    rank_projection = (jnp.dot(normalized_input, down_matrix, preferred_element_type=jnp.float32) * scale_coefficient).astype(jnp.bfloat16)
    value = (jnp.dot(normalized_input, value_weight, preferred_element_type=jnp.float32) + jnp.dot(rank_projection, up_matrix, preferred_element_type=jnp.float32)).astype(jnp.bfloat16)
    section_output = (widened + jnp.dot(value, out_weight, preferred_element_type=jnp.float32)).astype(jnp.bfloat16)
    return (section_output, normalized_input, rank_projection, inverse_root_mean)

def contract(left, right, left_dim, right_dim):
    return lax.dot_general(left, right, (((left_dim,), (right_dim,)), ((), ())), preferred_element_type=jnp.float32)

def section_backward_pass(layer_activation, incoming_gradient, norm_gains, value_weight, out_weight, down_matrix, up_matrix, scale_coefficient, normalized_input, rank_projection, inverse_root_mean):
    value_grad = contract(incoming_gradient, out_weight, 1, 1).astype(jnp.bfloat16)
    up_product = contract(rank_projection, value_grad, 0, 0)
    low_grad = (contract(value_grad, up_matrix, 1, 1) * scale_coefficient).astype(jnp.bfloat16)
    down_product = contract(normalized_input, low_grad, 0, 0)
    normed_grad = contract(value_grad, value_weight, 1, 1) + contract(low_grad, down_matrix, 1, 1)
    widened = layer_activation.astype(jnp.float32)
    scaled = normed_grad * norm_gains[None, :]
    cubed = inverse_root_mean * inverse_root_mean * inverse_root_mean
    input_grad = incoming_gradient.astype(jnp.float32) + inverse_root_mean[:, None] * scaled - widened * cubed[:, None] * lax.optimization_barrier(jnp.mean(widened * scaled, axis=-1, keepdims=True))
    return (input_grad.astype(jnp.bfloat16), down_product, up_product)

def reference(residual_input, output_gradient, value_projection_weight, output_weight, adapter_down_weight, adapter_up_weight, input_norm_scale, segment_adapter_index, adapter_rank_blocks):
    down_sums = [jnp.zeros((MODEL_WIDTH, PACKED_COLUMNS), jnp.float32) for layer_position in range(LAYER_SECTIONS)]
    up_sums = [jnp.zeros((PACKED_COLUMNS, VALUE_WIDTH), jnp.float32) for layer_position in range(LAYER_SECTIONS)]
    for micro_index in range(M):
        scale_coefficient = coefficients(segment_adapter_index[micro_index], adapter_rank_blocks)
        layer_activation = residual_input[micro_index]
        saved = []
        for layer_position in range(LAYER_SECTIONS):
            section_output, normalized_input, rank_projection, inverse_root_mean = section_forward_pass(layer_activation, input_norm_scale[layer_position], value_projection_weight[layer_position], output_weight[layer_position], adapter_down_weight[layer_position], adapter_up_weight[layer_position], scale_coefficient)
            saved.append((layer_activation, normalized_input, rank_projection, inverse_root_mean))
            layer_activation = section_output
        incoming_gradient = output_gradient[micro_index]
        for layer_position in reversed(range(LAYER_SECTIONS)):
            layer_activation, normalized_input, rank_projection, inverse_root_mean = saved[layer_position]
            incoming_gradient, down_product, up_product = section_backward_pass(layer_activation, incoming_gradient, input_norm_scale[layer_position], value_projection_weight[layer_position], output_weight[layer_position], adapter_down_weight[layer_position], adapter_up_weight[layer_position], scale_coefficient, normalized_input, rank_projection, inverse_root_mean)
            down_sums[layer_position] = down_sums[layer_position] + down_product
            up_sums[layer_position] = up_sums[layer_position] + up_product
    return (jnp.stack(down_sums), jnp.stack(up_sums))
```

```python
import jax
import jax.numpy as jnp
from jax import lax
from jax.sharding import Mesh, PartitionSpec as P

ADAPTERS = 4
EPSILON = 1e-06
ADAPTER_ALPHA = 32.0
BF = jnp.bfloat16
F32 = jnp.float32
GROUP = ("y", "z", "c")


def shifted(value, steps):
    count = lax.axis_size("x")
    return lax.ppermute(value, "x", [(j, (j + steps) % count) for j in range(count)])


def contract(left, right, left_dim, right_dim):
    return lax.dot_general(
        left, right, (((left_dim,), (right_dim,)), ((), ())), preferred_element_type=F32
    )


def split_pair(value):
    high = lax.reduce_precision(value, 8, 7)
    return high.astype(BF), (value - high).astype(BF)


def coefficient_row(adapter, adapter_rank_blocks, columns):
    rank_sizes = 8 * adapter_rank_blocks
    adapters = jnp.arange(ADAPTERS, dtype=jnp.int32)
    ends = jnp.sum(
        jnp.where(adapters[None, :] <= adapters[:, None], rank_sizes[None, :], 0), axis=1
    )
    column = jnp.arange(columns, dtype=jnp.int32)
    owner = jnp.sum((column[:, None] >= ends[None, :]).astype(jnp.int32), axis=1)
    rank = jnp.sum(jnp.where(adapters == adapter, rank_sizes, 0)).astype(F32)
    return jnp.where(owner == adapter, ADAPTER_ALPHA / rank, 0.0)[None, :]


def spread(quarter, position, groups, lanes):
    count = lax.axis_size("x")
    tokens = quarter.shape[0]
    columns = quarter.reshape(tokens, groups, count, lanes)
    blocks = []
    for k in range(count):
        piece = lax.dynamic_index_in_dim(columns, (position - k) % count, 2, keepdims=False)
        piece = piece.reshape(tokens, groups * lanes)
        blocks.append(shifted(piece, -k) if k else piece)
    return jnp.concatenate(blocks, axis=0)


def summed_over_x(partial, tokens):
    total = partial[:tokens].astype(F32)
    arrived = [
        shifted(partial[k * tokens : (k + 1) * tokens], k)
        for k in range(1, lax.axis_size("x"))
    ]
    for part in arrived:
        total = total + part.astype(F32)
    return total


def gathered_over_x(own):
    return jnp.concatenate(
        [own] + [shifted(own, -k) for k in range(1, lax.axis_size("x"))], axis=0
    )


def exchanged(value, axis):
    return lax.all_to_all(value, axis, split_axis=0, concat_axis=0, tiled=True).astype(F32).sum(
        axis=0
    )


def local(
    residual_input,
    output_gradient,
    value_projection_weight,
    output_weight,
    adapter_down_weight,
    adapter_up_weight,
    input_norm_scale,
    segment_adapter_index,
    adapter_rank_blocks,
):
    ny, nz, nx, nc = (lax.axis_size(name) for name in ("y", "z", "x", "c"))
    yi, zi, xi, ci = (lax.axis_index(name) for name in ("y", "z", "x", "c"))
    rows = value_projection_weight.shape[1]
    value_cols = value_projection_weight.shape[2]
    packed = adapter_down_weight.shape[2]
    width = adapter_down_weight.shape[1]
    both = value_cols + packed
    layers = ny
    depth = nz * nc * rows
    place = (zi * nx + xi) * nc + ci

    down_rows = lax.dynamic_slice(adapter_down_weight[0], (place * rows, 0), (rows, packed))
    in_local = jnp.concatenate([value_projection_weight[0], down_rows], axis=1)
    in_full = lax.all_gather(in_local, GROUP, axis=0, tiled=True).reshape(layers, depth, both)
    out_full = lax.all_gather(output_weight[0].T, GROUP, axis=0, tiled=True).reshape(
        layers, depth, value_cols
    )

    gains_local = lax.dynamic_index_in_dim(
        input_norm_scale.reshape(nz, nx, nc * rows), xi, 1, keepdims=False
    ).reshape(depth)
    gains = lax.all_gather(gains_local, "y", axis=0, tiled=False)
    ups = lax.all_gather(adapter_up_weight[0], "y", axis=0, tiled=False)

    all_tokens = residual_input.shape[0] * residual_input.shape[1]
    tokens = all_tokens // ny
    first = yi * tokens
    own_x = lax.dynamic_slice(residual_input.reshape(all_tokens, width), (first, 0), (tokens, width))
    own_g = lax.dynamic_slice(output_gradient.reshape(all_tokens, width), (first, 0), (tokens, width))
    adapter = lax.dynamic_index_in_dim(segment_adapter_index.reshape(ny), yi, 0, keepdims=False)
    coef = coefficient_row(adapter, adapter_rank_blocks, packed)

    state = spread(own_x, xi, nz, nc * rows)
    grad = spread(own_g, xi, nz, nc * rows)

    inputs, scaled, projected, inverse = [], [], [], []
    for layer in range(layers):
        widened = state.astype(F32)
        squares = jnp.sum(widened * widened, axis=-1, keepdims=True)
        scaled_input = (widened * gains[layer][None, :]).astype(BF)
        partial = contract(scaled_input, in_full[layer], 1, 0)
        high, low_part = split_pair(squares)
        sent = jnp.concatenate([partial.astype(BF), high, low_part], axis=1)
        total = summed_over_x(sent, tokens)
        mean = (total[:, both : both + 1] + total[:, both + 1 : both + 2]) / width
        inv = lax.rsqrt(mean + EPSILON)
        inputs.append(state)
        scaled.append(scaled_input)
        projected.append(total[:, :both])
        inverse.append(inv)
        if layer + 1 < layers:
            low = (total[:, value_cols:both] * inv * coef).astype(BF)
            value = (total[:, :value_cols] * inv + contract(low, ups[layer], 1, 0)).astype(BF)
            values = gathered_over_x(value)
            state = (widened + contract(values, out_full[layer], 1, 1)).astype(BF)

    downs, raised = [None] * layers, [None] * layers
    for layer in reversed(range(layers)):
        sent = contract(grad, out_full[layer], 1, 0).astype(BF)
        value_grad = summed_over_x(sent, tokens).astype(BF)
        low_grad = (contract(value_grad, ups[layer], 1, 1) * coef).astype(BF)
        inv = inverse[layer]
        wide_value, wide_low = value_grad.astype(F32), low_grad.astype(F32)
        low_hat = (projected[layer][:, value_cols:] * coef).astype(BF)
        own = [(wide_value * inv).astype(BF), (wide_low * inv).astype(BF), low_hat]
        if layer > 0:
            inner = jnp.sum(projected[layer][:, :value_cols] * wide_value, axis=1, keepdims=True)
            inner = inner + jnp.sum(
                projected[layer][:, value_cols:] * wide_low, axis=1, keepdims=True
            )
            own.extend(split_pair(inv * inv * inv * inner / width))
        arrived = gathered_over_x(jnp.concatenate(own, axis=1))
        mixed = arrived[:, :both]
        if layer > 0:
            start = both + packed
            kappa = arrived[:, start : start + 1].astype(F32) + arrived[
                :, start + 1 : start + 2
            ].astype(F32)
            back = contract(mixed, in_full[layer], 1, 1)
            grad = (
                grad.astype(F32)
                + gains[layer][None, :] * back
                - kappa * inputs[layer].astype(F32)
            ).astype(BF)
        downs[layer] = contract(mixed[:, value_cols:], scaled[layer], 0, 0)
        chosen = lax.dynamic_index_in_dim(
            mixed[:, :value_cols].reshape(mixed.shape[0], nz, nx, -1), xi, 2, keepdims=False
        ).reshape(mixed.shape[0], -1)
        raised[layer] = contract(chosen, arrived[:, both : both + packed], 0, 0)

    down = jnp.stack(downs).astype(BF).reshape(layers, packed, nz, nc, rows)
    down = down.transpose(3, 0, 2, 1, 4)
    up = jnp.stack(raised).reshape(layers, nz, nc, -1, packed).transpose(2, 0, 1, 3, 4)
    down, up = (exchanged(down, "c").astype(BF), exchanged(up, "c"))
    down, up = (exchanged(down, "y").astype(BF), exchanged(up, "y"))
    down, up = (exchanged(down, "z"), exchanged(up, "z"))
    return (down.T[None], up.T[None])


def solution(mesh):
    shape = mesh.devices.shape
    cores, across = 2, 4
    split = Mesh(
        mesh.devices.reshape(shape[0], shape[1] // (across * cores), across, cores),
        ("y", "z", "x", "c"),
    )
    fsdp = ("z", "x", "c")
    placed = (
        P(None, fsdp, None),
        P(None, fsdp, None),
        P("y", fsdp, None),
        P("y", None, fsdp),
        P("y", None, None),
        P("y", None, None),
        P("y", None),
        P(None, fsdp),
        P(),
    )
    return jax.shard_map(
        local,
        mesh=split,
        in_specs=placed,
        out_specs=(P("y", fsdp, None), P("y", None, fsdp)),
        check_vma=False,
    )
```

```python
import jax
import jax.numpy as jnp
from jax import lax
from jax.experimental.layout import Layout, with_layout_constraint
from jax.sharding import Mesh, PartitionSpec as P

ADAPTERS = 4
EPSILON = 1e-06
ADAPTER_ALPHA = 32.0
BF = jnp.bfloat16
F32 = jnp.float32
GROUP = ("y", "z", "c")


def contract(left, right, left_dim, right_dim):
    return lax.dot_general(
        left, right, (((left_dim,), (right_dim,)), ((), ())), preferred_element_type=F32
    )


def split_pair(value):
    high = lax.reduce_precision(value, 8, 7)
    return high.astype(BF), (value - high).astype(BF)


def coefficient_row(adapter, adapter_rank_blocks, columns):
    rank_sizes = 8 * adapter_rank_blocks
    adapters = jnp.arange(ADAPTERS, dtype=jnp.int32)
    ends = jnp.sum(
        jnp.where(adapters[None, :] <= adapters[:, None], rank_sizes[None, :], 0), axis=1
    )
    column = jnp.arange(columns, dtype=jnp.int32)
    owner = jnp.sum((column[:, None] >= ends[None, :]).astype(jnp.int32), axis=1)
    rank = jnp.sum(jnp.where(adapters == adapter, rank_sizes, 0)).astype(F32)
    return jnp.where(owner == adapter, ADAPTER_ALPHA / rank, 0.0)[None, :]


def exchanged(value, axis):
    return lax.all_to_all(value, axis, split_axis=0, concat_axis=0, tiled=True)


def summed(value):
    return value.astype(F32).sum(axis=0)


def gathered_sum(partial):
    return summed(lax.all_gather(partial, "x", axis=0, tiled=False))


def local(
    residual_input,
    output_gradient,
    value_projection_weight,
    output_weight,
    adapter_down_weight,
    adapter_up_weight,
    input_norm_scale,
    segment_adapter_index,
    adapter_rank_blocks,
):
    ny, nz, nx, nc = (lax.axis_size(name) for name in ("y", "z", "x", "c"))
    yi, zi, xi, ci = (lax.axis_index(name) for name in ("y", "z", "x", "c"))
    rows = value_projection_weight.shape[1]
    value_cols = value_projection_weight.shape[2]
    packed = adapter_down_weight.shape[2]
    width = adapter_down_weight.shape[1]
    both = value_cols + packed
    layers = ny
    lanes = nc * rows
    depth = nz * lanes

    joined = jnp.concatenate([value_projection_weight[0], output_weight[0].T], axis=1)
    joined = with_layout_constraint(joined, Layout(major_to_minor=(0, 1)))
    full = lax.all_gather(joined, GROUP, axis=0, tiled=False)
    full = with_layout_constraint(full, Layout(major_to_minor=(0, 1, 2)))
    full = full.reshape(layers, depth, 2 * value_cols)
    value_full = [full[layer, :, :value_cols] for layer in range(layers)]
    out_full = [full[layer, :, value_cols:] for layer in range(layers)]

    all_tokens = residual_input.shape[0] * residual_input.shape[1]
    tokens = all_tokens // ny
    first = yi * tokens
    own = jnp.stack(
        [
            lax.dynamic_slice(array.reshape(all_tokens, width), (first, 0), (tokens, width))
            for array in (residual_input, output_gradient)
        ]
    )
    own = own.reshape(2, tokens, nz, nx, lanes).transpose(3, 0, 1, 2, 4)
    spread = exchanged(own.reshape(nx, 2, tokens, depth), "x")
    state = spread[:, 0].reshape(nx * tokens, depth)
    grad = spread[:, 1].reshape(nx * tokens, depth)

    down_local = lax.dynamic_index_in_dim(
        adapter_down_weight[0].T.reshape(packed, nz, nx, lanes), xi, 2, keepdims=False
    ).reshape(1, packed, depth)
    downs_full = exchanged(jnp.broadcast_to(down_local, (layers, packed, depth)), "y")

    gains_local = lax.dynamic_index_in_dim(
        input_norm_scale.reshape(nz, nx, lanes), xi, 1, keepdims=False
    ).reshape(depth)
    gains = lax.all_gather(gains_local, "y", axis=0, tiled=False)
    ups = lax.all_gather(adapter_up_weight[0], "y", axis=0, tiled=False)
    adapter = lax.dynamic_index_in_dim(segment_adapter_index.reshape(ny), yi, 0, keepdims=False)
    coef_row = coefficient_row(adapter, adapter_rank_blocks, packed)
    coef = lax.all_gather(
        jnp.broadcast_to(coef_row, (tokens, packed)), "x", axis=0, tiled=True
    )

    chunk = value_cols // layers
    last = contract(grad, out_full[layers - 1], 1, 0).astype(BF)
    inputs, scaled, projected, inverse, last_sum = [], [], [], [], []
    for layer in range(layers):
        widened = state.astype(F32)
        squares = jnp.sum(widened * widened, axis=-1, keepdims=True)
        scaled_input = (widened * gains[layer][None, :]).astype(BF)
        high, low_part = split_pair(squares)
        total = gathered_sum(
            jnp.concatenate(
                [
                    contract(scaled_input, value_full[layer], 1, 0).astype(BF),
                    last[:, layer * chunk : (layer + 1) * chunk],
                    contract(scaled_input, downs_full[layer], 1, 1).astype(BF),
                    high,
                    low_part,
                ],
                axis=1,
            )
        )
        side = value_cols + chunk
        mean = (total[:, side + packed : side + packed + 1] + total[:, side + packed + 1 :]) / width
        inv = lax.rsqrt(mean + EPSILON)
        value_part, low_piece = total[:, :value_cols], total[:, side : side + packed]
        inputs.append(state)
        scaled.append(scaled_input)
        projected.append((value_part, low_piece))
        inverse.append(inv)
        last_sum.append(total[:, value_cols:side])
        if layer + 1 < layers:
            low = (low_piece * inv * coef).astype(BF)
            value = (value_part * inv + contract(low, ups[layer], 1, 0)).astype(BF)
            state = (widened + contract(value, out_full[layer], 1, 1)).astype(BF)

    blocks = [None] * layers
    extra = -(-packed // rows)
    for layer in reversed(range(layers)):
        if layer + 1 < layers:
            value_sum = gathered_sum(contract(grad, out_full[layer], 1, 0).astype(BF))
        else:
            value_sum = jnp.concatenate(last_sum, axis=1)
        value_grad = value_sum.astype(BF)
        low_grad = (contract(value_grad, ups[layer], 1, 1) * coef).astype(BF)
        inv = inverse[layer]
        value_part, low_piece = projected[layer]
        wide_value, wide_low = value_grad.astype(F32), low_grad.astype(F32)
        mixed_value, mixed_low = (wide_value * inv).astype(BF), (wide_low * inv).astype(BF)
        if layer > 0:
            inner = jnp.sum(value_part * wide_value, axis=1, keepdims=True)
            inner = inner + jnp.sum(low_piece * wide_low, axis=1, keepdims=True)
            kappa = inv * inv * inv * inner / width
            back = contract(mixed_value, value_full[layer], 1, 1)
            back = back + contract(mixed_low, downs_full[layer], 1, 0)
            grad = (
                grad.astype(F32)
                + gains[layer][None, :] * back
                - kappa * inputs[layer].astype(F32)
            ).astype(BF)
        down = contract(mixed_low, scaled[layer], 0, 0)
        down = down.reshape(packed, nz, nc, rows).transpose(2, 1, 0, 3)
        low = (low_piece * inv * coef).astype(BF)
        chosen = lax.dynamic_index_in_dim(
            value_grad.reshape(nx * tokens, nz, nx, -1), xi, 2, keepdims=False
        )
        each = chosen.shape[2] // nc
        up = contract(chosen.reshape(nx * tokens, -1), low, 0, 0)
        up = up.reshape(nz, nc, each, packed).transpose(1, 0, 2, 3)
        up = jnp.pad(up, ((0, 0), (0, 0), (0, 0), (0, extra * rows - packed)))
        block = jnp.concatenate(
            [down] + [up[..., k * rows : (k + 1) * rows] for k in range(extra)], axis=2
        ).astype(BF)
        blocks[layer] = summed(exchanged(block, "c")).astype(BF)

    total = summed(exchanged(jnp.stack(blocks), "y")).astype(BF)
    total = summed(exchanged(total, "z"))
    up = jnp.concatenate(
        [total[packed + k * each : packed + (k + 1) * each] for k in range(extra)], axis=1
    )[:, :packed]
    return (total[:packed].T[None], up.T[None])


def solution(mesh):
    shape = mesh.devices.shape
    cores, across = 2, 4
    split = Mesh(
        mesh.devices.reshape(shape[0], shape[1] // (across * cores), across, cores),
        ("y", "z", "x", "c"),
    )
    fsdp = ("z", "x", "c")
    placed = (
        P(None, fsdp, None),
        P(None, fsdp, None),
        P("y", fsdp, None),
        P("y", None, fsdp),
        P("y", None, None),
        P("y", None, None),
        P("y", None),
        P(None, fsdp),
        P(),
    )
    return jax.shard_map(
        local,
        mesh=split,
        in_specs=placed,
        out_specs=(P("y", fsdp, None), P("y", None, fsdp)),
        check_vma=False,
    )
```

```python
import functools

import jax
import jax.numpy as jnp
from jax import lax
from jax.experimental import pallas as pl
from jax.experimental.layout import Layout, with_layout_constraint
from jax.experimental.pallas import tpu as pltpu
from jax.sharding import Mesh, PartitionSpec as P

ADAPTERS = 4
EPSILON = 1e-06
ADAPTER_ALPHA = 32.0
BF = jnp.bfloat16
F32 = jnp.float32
GROUP = ("y", "z", "c")
LANES = 128
STEP = 512
INTERPRET = False


def contract(left, right, left_dim, right_dim):
    return lax.dot_general(
        left, right, (((left_dim,), (right_dim,)), ((), ())), preferred_element_type=F32
    )


def coefficient_row(adapter, adapter_rank_blocks, packed, columns):
    rank_sizes = 8 * adapter_rank_blocks
    adapters = jnp.arange(ADAPTERS, dtype=jnp.int32)
    ends = jnp.sum(
        jnp.where(adapters[None, :] <= adapters[:, None], rank_sizes[None, :], 0), axis=1
    )
    column = jnp.arange(columns, dtype=jnp.int32)
    owner = jnp.sum((column[:, None] >= ends[None, :]).astype(jnp.int32), axis=1)
    rank = jnp.sum(jnp.where(adapters == adapter, rank_sizes, 0)).astype(F32)
    held = (owner == adapter) & (column < packed)
    return jnp.where(held, ADAPTER_ALPHA / rank, 0.0)[None, :]


def exchanged(value, axis):
    return lax.all_to_all(value, axis, split_axis=0, concat_axis=0, tiled=True)


def summed(value):
    return value.astype(F32).sum(axis=0)


def gathered(partial):
    return lax.all_gather(partial, "x", axis=0, tiled=False)


def token_stats(gathered_ref, value_cols, chunk, packed, width):
    total = gathered_ref[...].astype(F32).sum(axis=0)
    side = total[:, value_cols + chunk :]
    mean = (side[:, packed : packed + 1] + side[:, packed + 1 : packed + 2]) / width
    return total[:, :value_cols], side, lax.rsqrt(mean + EPSILON)


def forward_kernel(*refs, first, sizes):
    value_cols, chunk, packed, width = sizes
    if first:
        grad, last_out, state, value_w, down_w, gain, sent, last_sum, scaled = refs[:9]
        acc, side_acc, square_acc, last_acc = refs[9:]
    else:
        before, coef, up, state, out_w, value_w, down_w, gain, last_piece = refs[:9]
        sent, new_state, scaled = refs[9:12]
        acc, side_acc, square_acc, values = refs[12:]
    step = pl.program_id(0)

    @pl.when(step == 0)
    def _():
        acc[...] = jnp.zeros_like(acc)
        side_acc[...] = jnp.zeros_like(side_acc)
        square_acc[...] = jnp.zeros_like(square_acc)
        if first:
            last_acc[...] = jnp.zeros_like(last_acc)
        else:
            value_part, side, inv = token_stats(before, value_cols, chunk, packed, width)
            low = (side * inv * coef[...]).astype(BF)
            values[...] = (value_part * inv + contract(low, up[0], 1, 0)).astype(BF)

    if first:
        wide = state[...].astype(F32)
        last_acc[...] += contract(grad[...], last_out[0], 1, 0)
    else:
        wide = state[...].astype(F32) + contract(values[...], out_w[0], 1, 1)
        new_state[...] = wide.astype(BF)
        wide = new_state[...].astype(F32)
    square_acc[...] += jnp.sum(wide * wide, axis=1, keepdims=True)
    scaled_input = (wide * gain[0]).astype(BF)
    scaled[...] = scaled_input
    acc[...] += contract(scaled_input, value_w[0], 1, 0)
    side_acc[...] += contract(scaled_input, down_w[0], 1, 1)

    @pl.when(step == pl.num_programs(0) - 1)
    def _():
        sent[:, :value_cols] = acc[...].astype(BF)
        if first:
            last = last_acc[...].astype(BF)
            last_sum[...] = last
            sent[:, value_cols : value_cols + chunk] = last[:, :chunk]
        else:
            sent[:, value_cols : value_cols + chunk] = last_piece[...]
        squares = square_acc[:, :1]
        high = squares.astype(BF).astype(F32)
        lane = lax.broadcasted_iota(jnp.int32, side_acc.shape, 1)
        side = jnp.where(lane == packed, high, side_acc[...])
        side = jnp.where(lane == packed + 1, squares - high, side)
        sent[:, value_cols + chunk :] = side.astype(BF)


def backward_kernel(*refs, last, bottom, sizes, spots):
    value_cols, chunk, packed, width = sizes
    nz, nx, nc, each = spots
    refs = list(refs)
    take = lambda n: [refs.pop(0) for _ in range(n)]
    where, = take(1)
    pieces = take(value_cols // chunk if last else 1)
    before, coef, up, scaled = take(4)
    if not bottom:
        state, grad, value_w, down_w, gain, out_w = take(6)
    own, other = take(2)
    if not bottom:
        sent, new_grad = take(2)
    mixed_low, raised = take(2)
    if not bottom:
        mixed_value, kappa, acc = take(3)
    step = pl.program_id(0)
    xi, ci = where[0], where[1]

    @pl.when(step == 0)
    def _():
        summed_pieces = [piece[...].astype(F32).sum(axis=0) for piece in pieces]
        total = summed_pieces[0] if len(pieces) == 1 else jnp.concatenate(summed_pieces, axis=1)
        value_grad = total.astype(BF)
        wide_value = value_grad.astype(F32)
        low_grad = (contract(value_grad, up[0], 1, 1) * coef[...]).astype(BF)
        wide_low = low_grad.astype(F32)
        value_part, side, inv = token_stats(before, value_cols, chunk, packed, width)
        mixed_low[...] = (wide_low * inv).astype(BF)
        if not bottom:
            mixed_value[...] = (wide_value * inv).astype(BF)
            inner = jnp.sum(value_part * wide_value, axis=1, keepdims=True)
            inner = inner + jnp.sum(side * wide_low, axis=1, keepdims=True)
            kappa[...] = jnp.broadcast_to(inv * inv * inv * inner / width, kappa.shape)
            acc[...] = jnp.zeros_like(acc)
        low = (side * inv * coef[...]).astype(BF)
        raised[...] = contract(value_grad, low, 0, 0)
        for z in range(nz):
            for target, core in ((own, ci), (other, 1 - ci)):
                row = pl.multiple_of((z * nx + xi) * nc * each + core * each, each)
                piece = raised[pl.ds(row, each), :]
                target[z, packed:, :] = jnp.concatenate(
                    [piece[:, k * LANES : (k + 1) * LANES] for k in range(piece.shape[1] // LANES)],
                    axis=0,
                ).astype(BF)

    lowered = contract(mixed_low[...], scaled[...], 0, 0)[:packed]
    per_step = scaled.shape[1] // (nc * LANES)
    for k in range(per_step):
        start = k * nc * LANES
        one = lowered[:, start : start + LANES]
        two = lowered[:, start + LANES : start + 2 * LANES]
        own[step * per_step + k, :packed, :] = jnp.where(ci == 0, one, two).astype(BF)
        other[step * per_step + k, :packed, :] = jnp.where(ci == 0, two, one).astype(BF)
    if not bottom:
        back = contract(mixed_value[...], value_w[0], 1, 1)
        back = back + contract(mixed_low[...], down_w[0], 1, 0)
        wide = grad[...].astype(F32) + gain[0] * back - kappa[:, :1] * state[...].astype(F32)
        updated = wide.astype(BF)
        new_grad[...] = updated
        acc[...] += contract(updated, out_w[0], 1, 0)

        @pl.when(step == pl.num_programs(0) - 1)
        def _():
            sent[...] = acc[...].astype(BF)


def whole(shape):
    return pl.BlockSpec(shape, lambda i: (0,) * len(shape))


def columns(tokens):
    return pl.BlockSpec((tokens, STEP), lambda i: (0, i))


def weight(layer, half, cols):
    return pl.BlockSpec((1, STEP, cols), lambda i: (layer, i, half))


def layered(layer, shape):
    return pl.BlockSpec((1,) + shape, lambda i: (layer,) + (0,) * len(shape))


def along(layer, rows):
    return pl.BlockSpec((1, rows, STEP), lambda i: (layer, 0, i))


def local(
    residual_input,
    output_gradient,
    value_projection_weight,
    output_weight,
    adapter_down_weight,
    adapter_up_weight,
    input_norm_scale,
    segment_adapter_index,
    adapter_rank_blocks,
):
    ny, nz, nx, nc = (lax.axis_size(name) for name in ("y", "z", "x", "c"))
    yi, zi, xi, ci = (lax.axis_index(name) for name in ("y", "z", "x", "c"))
    rows = value_projection_weight.shape[1]
    value_cols = value_projection_weight.shape[2]
    packed = adapter_down_weight.shape[2]
    width = adapter_down_weight.shape[1]
    both = value_cols + packed
    layers = ny
    lanes = nc * rows
    depth = nz * lanes

    joined = jnp.concatenate([value_projection_weight[0], output_weight[0].T], axis=1)
    joined = with_layout_constraint(joined, Layout(major_to_minor=(0, 1)))
    full = lax.all_gather(joined, GROUP, axis=0, tiled=False)
    full = with_layout_constraint(full, Layout(major_to_minor=(0, 1, 2)))
    full = full.reshape(layers, depth, 2 * value_cols)

    all_tokens = residual_input.shape[0] * residual_input.shape[1]
    tokens = all_tokens // ny
    first = yi * tokens
    own = jnp.stack(
        [
            lax.dynamic_slice(array.reshape(all_tokens, width), (first, 0), (tokens, width))
            for array in (residual_input, output_gradient)
        ]
    )
    own = own.reshape(2, tokens, nz, nx, lanes).transpose(3, 0, 1, 2, 4)
    spread = exchanged(own.reshape(nx, 2, tokens, depth), "x")
    state = spread[:, 0].reshape(nx * tokens, depth)
    grad = spread[:, 1].reshape(nx * tokens, depth)

    down_local = lax.dynamic_index_in_dim(
        adapter_down_weight[0].T.reshape(packed, nz, nx, lanes), xi, 2, keepdims=False
    ).reshape(1, packed, depth)
    downs_full = exchanged(jnp.broadcast_to(down_local, (layers, packed, depth)), "y")
    padded = -(-packed // LANES) * LANES
    downs_full = jnp.pad(downs_full, ((0, 0), (0, padded - packed), (0, 0)))

    gains_local = lax.dynamic_index_in_dim(
        input_norm_scale.reshape(nz, nx, lanes), xi, 1, keepdims=False
    ).reshape(depth)
    gains = lax.all_gather(gains_local, "y", axis=0, tiled=False)
    gains = gains.reshape(layers, 1, depth)
    ups = lax.all_gather(adapter_up_weight[0], "y", axis=0, tiled=False)
    ups = jnp.pad(ups, ((0, 0), (0, padded - packed), (0, 0)))
    adapter = lax.dynamic_index_in_dim(segment_adapter_index.reshape(ny), yi, 0, keepdims=False)
    coef_row = coefficient_row(adapter, adapter_rank_blocks, packed, padded)
    coef = lax.all_gather(
        jnp.broadcast_to(coef_row, (tokens, padded)), "x", axis=0, tiled=True
    )

    count = nx * tokens
    chunk = value_cols // layers
    sizes = (value_cols, chunk, packed, width)
    wire = value_cols + chunk + padded
    each = value_cols // (nz * nx * nc)
    steps = depth // STEP
    shape = jax.ShapeDtypeStruct
    call = functools.partial(pl.pallas_call, grid=(steps,), interpret=INTERPRET)
    sent_shape, wide_shape = shape((count, wire), BF), shape((count, depth), BF)
    sums = [
        pltpu.VMEM((count, value_cols), F32),
        pltpu.VMEM((count, padded), F32),
        pltpu.VMEM((count, LANES), F32),
    ]
    top = layers - 1

    sent, last, scaled_input = call(
        functools.partial(forward_kernel, first=True, sizes=sizes),
        out_shape=(sent_shape, shape((count, value_cols), BF), wide_shape),
        in_specs=[
            columns(count),
            weight(top, 1, value_cols),
            columns(count),
            weight(0, 0, value_cols),
            along(0, padded),
            along(0, 1),
        ],
        out_specs=(whole((count, wire)), whole((count, value_cols)), columns(count)),
        scratch_shapes=sums + [pltpu.VMEM((count, value_cols), F32)],
    )(grad, full, state, full, downs_full, gains)
    arrived, inputs, scaled = [gathered(sent)], [state], [scaled_input]
    for layer in range(1, layers):
        sent, state, scaled_input = call(
            functools.partial(forward_kernel, first=False, sizes=sizes),
            out_shape=(sent_shape, wide_shape, wide_shape),
            in_specs=[
                whole((nx, count, wire)),
                whole((count, padded)),
                layered(layer - 1, (padded, value_cols)),
                columns(count),
                weight(layer - 1, 1, value_cols),
                weight(layer, 0, value_cols),
                along(layer, padded),
                along(layer, 1),
                pl.BlockSpec((count, chunk), lambda i, layer=layer: (0, layer)),
            ],
            out_specs=(whole((count, wire)), columns(count), columns(count)),
            scratch_shapes=sums + [pltpu.VMEM((count, value_cols), BF)],
        )(arrived[-1], coef, ups, state, full, full, downs_full, gains, last)
        arrived.append(gathered(sent))
        inputs.append(state)
        scaled.append(scaled_input)

    spots = (nz, nx, nc, each)
    place_ids = jnp.stack([xi, ci]).astype(jnp.int32)
    block_rows = packed + each * (padded // LANES)
    block_shape = (nz, block_rows, LANES)
    kept, crossed = [None] * layers, [None] * layers
    pieces, piece_specs = arrived, [
        pl.BlockSpec((nx, count, chunk), lambda i: (0, 0, value_cols // chunk))
    ] * layers
    for layer in reversed(range(layers)):
        bottom = layer == 0
        operands = [place_ids, *pieces, arrived[layer], coef, ups, scaled[layer]]
        specs = [
            pl.BlockSpec(memory_space=pltpu.SMEM),
            *piece_specs,
            whole((nx, count, wire)),
            whole((count, padded)),
            layered(layer, (padded, value_cols)),
            columns(count),
        ]
        outs = [shape(block_shape, BF)] * 2
        out_specs = [whole(block_shape)] * 2
        scratch = [pltpu.VMEM((count, padded), BF), pltpu.VMEM((value_cols, padded), F32)]
        if not bottom:
            operands += [inputs[layer], grad, full, downs_full, gains, full]
            specs += [
                columns(count),
                columns(count),
                weight(layer, 0, value_cols),
                along(layer, padded),
                along(layer, 1),
                weight(layer - 1, 1, value_cols),
            ]
            outs += [shape((count, value_cols), BF), wide_shape]
            out_specs += [whole((count, value_cols)), columns(count)]
            scratch += [
                pltpu.VMEM((count, value_cols), BF),
                pltpu.VMEM((count, LANES), F32),
                pltpu.VMEM((count, value_cols), F32),
            ]
        results = call(
            functools.partial(
                backward_kernel, last=layer == top, bottom=bottom, sizes=sizes, spots=spots
            ),
            out_shape=outs,
            in_specs=specs,
            out_specs=out_specs,
            scratch_shapes=scratch,
        )(*operands)
        kept[layer] = results[0]
        crossed[layer] = lax.ppermute(results[1], "c", [(j, 1 - j) for j in range(nc)])
        if not bottom:
            grad = results[3]
            pieces = [gathered(results[2])]
            piece_specs = [whole((nx, count, value_cols))]

    total = (jnp.stack(kept).astype(F32) + jnp.stack(crossed).astype(F32)).astype(BF)
    total = summed(exchanged(total, "y")).astype(BF)
    total = summed(exchanged(total, "z"))
    up = jnp.concatenate(
        [total[packed + k * each : packed + (k + 1) * each] for k in range(padded // LANES)],
        axis=1,
    )[:, :packed]
    return (total[:packed].T[None], up.T[None])


def solution(mesh):
    shape = mesh.devices.shape
    cores, across = 2, 4
    split = Mesh(
        mesh.devices.reshape(shape[0], shape[1] // (across * cores), across, cores),
        ("y", "z", "x", "c"),
    )
    fsdp = ("z", "x", "c")
    placed = (
        P(None, fsdp, None),
        P(None, fsdp, None),
        P("y", fsdp, None),
        P("y", None, fsdp),
        P("y", None, None),
        P("y", None, None),
        P("y", None),
        P(None, fsdp),
        P(),
    )
    return jax.shard_map(
        local,
        mesh=split,
        in_specs=placed,
        out_specs=(P("y", fsdp, None), P("y", None, fsdp)),
        check_vma=False,
    )
```

```python
import functools

import jax
import jax.numpy as jnp
from jax import lax
from jax.experimental import pallas as pl
from jax.experimental.layout import Layout, with_layout_constraint
from jax.experimental.pallas import tpu as pltpu
from jax.sharding import Mesh, PartitionSpec as P

ADAPTERS = 4
EPSILON = 1e-06
ADAPTER_ALPHA = 32.0
BF = jnp.bfloat16
F32 = jnp.float32
GROUP = ("y", "z", "c")
LANES = 128
STEP = 512
INTERPRET = False
KERNEL_BYTES = 50 * 1024 * 1024


def contract(left, right, left_dim, right_dim):
    return lax.dot_general(
        left, right, (((left_dim,), (right_dim,)), ((), ())), preferred_element_type=F32
    )


def coefficient_row(adapter, adapter_rank_blocks, packed, columns):
    rank_sizes = 8 * adapter_rank_blocks
    adapters = jnp.arange(ADAPTERS, dtype=jnp.int32)
    ends = jnp.sum(
        jnp.where(adapters[None, :] <= adapters[:, None], rank_sizes[None, :], 0), axis=1
    )
    column = jnp.arange(columns, dtype=jnp.int32)
    owner = jnp.sum((column[:, None] >= ends[None, :]).astype(jnp.int32), axis=1)
    rank = jnp.sum(jnp.where(adapters == adapter, rank_sizes, 0)).astype(F32)
    held = (owner == adapter) & (column < packed)
    return jnp.where(held, ADAPTER_ALPHA / rank, 0.0)[None, :]


def exchanged(value, axis):
    return lax.all_to_all(value, axis, split_axis=0, concat_axis=0, tiled=True)


def summed(value):
    return value.astype(F32).sum(axis=0)


def gathered(partial):
    return lax.all_gather(partial, "x", axis=0, tiled=False)


def token_stats(gathered_ref, value_cols, chunk, packed, width):
    total = gathered_ref[...].astype(F32).sum(axis=0)
    side = total[:, value_cols + chunk :]
    mean = (side[:, packed : packed + 1] + side[:, packed + 1 : packed + 2]) / width
    return total[:, :value_cols], side, lax.rsqrt(mean + EPSILON)


def forward_kernel(*refs, layer, sizes):
    value_cols, chunk, packed, width = sizes
    first = layer == 0
    if first:
        grad, last_out, state, value_w, down_w, gain, sent, last_sum, scaled = refs[:9]
        acc, side_acc, square_acc, last_acc = refs[9:]
    else:
        before, coef, up, state, out_w, value_w, down_w, gain, last_piece = refs[:9]
        sent, new_state, scaled = refs[9:12]
        acc, side_acc, square_acc, values = refs[12:]
    step = pl.program_id(0)

    @pl.when(step == 0)
    def _():
        acc[...] = jnp.zeros_like(acc)
        side_acc[...] = jnp.zeros_like(side_acc)
        square_acc[...] = jnp.zeros_like(square_acc)
        if first:
            last_acc[...] = jnp.zeros_like(last_acc)
        else:
            value_part, side, inv = token_stats(before, value_cols, chunk, packed, width)
            low = (side * inv * coef[...]).astype(BF)
            values[...] = (value_part * inv + contract(low, up[layer - 1], 1, 0)).astype(BF)

    if first:
        wide = state[...].astype(F32)
        last_acc[...] += contract(grad[...], last_out[0], 1, 0)
    else:
        wide = state[...].astype(F32) + contract(values[...], out_w[0], 1, 1)
        new_state[...] = wide.astype(BF)
        wide = new_state[...].astype(F32)
    square_acc[...] += jnp.sum(wide * wide, axis=1, keepdims=True)
    scaled_input = (wide * gain[0]).astype(BF)
    scaled[...] = scaled_input
    acc[...] += contract(scaled_input, value_w[0], 1, 0)
    side_acc[...] += contract(scaled_input, down_w[0], 1, 1)

    @pl.when(step == pl.num_programs(0) - 1)
    def _():
        sent[:, :value_cols] = acc[...].astype(BF)
        if first:
            last = last_acc[...].astype(BF)
            last_sum[...] = last
            sent[:, value_cols : value_cols + chunk] = last[:, :chunk]
        else:
            sent[:, value_cols : value_cols + chunk] = last_piece[
                :, layer * chunk : (layer + 1) * chunk
            ]
        squares = square_acc[:, :1]
        high = squares.astype(BF).astype(F32)
        lane = lax.broadcasted_iota(jnp.int32, side_acc.shape, 1)
        side = jnp.where(lane == packed, high, side_acc[...])
        side = jnp.where(lane == packed + 1, squares - high, side)
        sent[:, value_cols + chunk :] = side.astype(BF)


def backward_kernel(*refs, layer, last, sizes, spots):
    value_cols, chunk, packed, width = sizes
    bottom = layer == 0
    nz, nx, nc, each = spots
    refs = list(refs)
    take = lambda n: [refs.pop(0) for _ in range(n)]
    where, = take(1)
    pieces = take(value_cols // chunk if last else 1)
    before, coef, up, scaled = take(4)
    if not bottom:
        state, grad, value_w, down_w, gain, out_w = take(6)
    own, other = take(2)
    if not bottom:
        sent, new_grad = take(2)
    mixed_low, raised = take(2)
    if not bottom:
        mixed_value, kappa, acc = take(3)
    step = pl.program_id(0)
    xi, ci = where[0], where[1]

    @pl.when(step == 0)
    def _():
        first = value_cols if last else 0
        wide = chunk if last else value_cols
        summed_pieces = [
            piece[:, :, first : first + wide].astype(F32).sum(axis=0) for piece in pieces
        ]
        total = summed_pieces[0] if len(pieces) == 1 else jnp.concatenate(summed_pieces, axis=1)
        value_grad = total.astype(BF)
        wide_value = value_grad.astype(F32)
        low_grad = (contract(value_grad, up[layer], 1, 1) * coef[...]).astype(BF)
        wide_low = low_grad.astype(F32)
        value_part, side, inv = token_stats(before, value_cols, chunk, packed, width)
        mixed_low[...] = (wide_low * inv).astype(BF)
        if not bottom:
            mixed_value[...] = (wide_value * inv).astype(BF)
            inner = jnp.sum(value_part * wide_value, axis=1, keepdims=True)
            inner = inner + jnp.sum(side * wide_low, axis=1, keepdims=True)
            kappa[...] = jnp.broadcast_to(inv * inv * inv * inner / width, kappa.shape)
            acc[...] = jnp.zeros_like(acc)
        low = (side * inv * coef[...]).astype(BF)
        raised[...] = contract(value_grad, low, 0, 0)
        for z in range(nz):
            for target, core in ((own, ci), (other, 1 - ci)):
                row = pl.multiple_of((z * nx + xi) * nc * each + core * each, each)
                piece = raised[pl.ds(row, each), :]
                target[z, packed:, :] = jnp.concatenate(
                    [piece[:, k * LANES : (k + 1) * LANES] for k in range(piece.shape[1] // LANES)],
                    axis=0,
                ).astype(BF)

    lowered = contract(mixed_low[...], scaled[...], 0, 0)[:packed]
    per_step = scaled.shape[1] // (nc * LANES)
    for k in range(per_step):
        start = k * nc * LANES
        one = lowered[:, start : start + LANES]
        two = lowered[:, start + LANES : start + 2 * LANES]
        own[step * per_step + k, :packed, :] = jnp.where(ci == 0, one, two).astype(BF)
        other[step * per_step + k, :packed, :] = jnp.where(ci == 0, two, one).astype(BF)
    if not bottom:
        back = contract(mixed_value[...], value_w[0], 1, 1)
        back = back + contract(mixed_low[...], down_w[0], 1, 0)
        wide = grad[...].astype(F32) + gain[0] * back - kappa[:, :1] * state[...].astype(F32)
        updated = wide.astype(BF)
        new_grad[...] = updated
        acc[...] += contract(updated, out_w[0], 1, 0)

        @pl.when(step == pl.num_programs(0) - 1)
        def _():
            sent[...] = acc[...].astype(BF)


def whole():
    return pl.BlockSpec(memory_space=pltpu.VMEM)


def columns(tokens):
    return pl.BlockSpec((tokens, STEP), lambda i: (0, i))


def weight(layer, half, cols):
    return pl.BlockSpec((1, STEP, cols), lambda i: (layer, i, half))


def along(layer, rows):
    return pl.BlockSpec((1, rows, STEP), lambda i: (layer, 0, i))


def local(
    residual_input,
    output_gradient,
    value_projection_weight,
    output_weight,
    adapter_down_weight,
    adapter_up_weight,
    input_norm_scale,
    segment_adapter_index,
    adapter_rank_blocks,
):
    ny, nz, nx, nc = (lax.axis_size(name) for name in ("y", "z", "x", "c"))
    yi, zi, xi, ci = (lax.axis_index(name) for name in ("y", "z", "x", "c"))
    rows = value_projection_weight.shape[1]
    value_cols = value_projection_weight.shape[2]
    packed = adapter_down_weight.shape[2]
    width = adapter_down_weight.shape[1]
    both = value_cols + packed
    layers = ny
    lanes = nc * rows
    depth = nz * lanes

    joined = jnp.concatenate([value_projection_weight[0], output_weight[0].T], axis=1)
    joined = with_layout_constraint(joined, Layout(major_to_minor=(0, 1)))
    full = lax.all_gather(joined, GROUP, axis=0, tiled=False)
    full = with_layout_constraint(full, Layout(major_to_minor=(0, 1, 2)))
    full = full.reshape(layers, depth, 2 * value_cols)

    all_tokens = residual_input.shape[0] * residual_input.shape[1]
    tokens = all_tokens // ny
    first = yi * tokens
    own = jnp.stack(
        [
            lax.dynamic_slice(array.reshape(all_tokens, width), (first, 0), (tokens, width))
            for array in (residual_input, output_gradient)
        ]
    )
    own = own.reshape(2, tokens, nz, nx, lanes).transpose(3, 0, 1, 2, 4)
    spread = exchanged(own.reshape(nx, 2, tokens, depth), "x")
    state = spread[:, 0].reshape(nx * tokens, depth)
    grad = spread[:, 1].reshape(nx * tokens, depth)

    padded = -(-packed // LANES) * LANES
    half = packed // nc
    down_half = lax.dynamic_slice(
        adapter_down_weight[0].T.reshape(packed, nz, nx, lanes),
        (ci * half, 0, xi, 0),
        (half, nz, 1, lanes),
    ).reshape(1, half, depth)
    mine = exchanged(jnp.broadcast_to(down_half, (layers, half, depth)), "y")
    theirs = lax.ppermute(mine, "c", [(j, 1 - j) for j in range(nc)])
    ordered = [jnp.where(ci == 0, mine, theirs), jnp.where(ci == 0, theirs, mine)]
    filler = jnp.zeros((layers, padded - packed, depth), BF)
    downs_full = jnp.concatenate(ordered + [filler], axis=1)

    gain_own = lax.dynamic_index_in_dim(
        input_norm_scale.reshape(nz, nx, lanes), xi, 1, keepdims=False
    ).reshape(depth // value_cols, value_cols)
    high = lax.reduce_precision(gain_own, 8, 7)
    middle = lax.reduce_precision(gain_own - high, 8, 7)
    parts = [high, middle, gain_own - high - middle]
    small = jnp.concatenate([adapter_up_weight[0]] + [part.astype(BF) for part in parts], axis=0)
    small = lax.all_gather(small, "y", axis=0, tiled=False)
    ups = jnp.pad(small[:, :packed], ((0, 0), (0, padded - packed), (0, 0)))
    gains = small[:, packed:].astype(F32).reshape(layers, 3, 1, depth)
    gains = gains[:, 0] + gains[:, 1] + gains[:, 2]
    adapter = lax.dynamic_index_in_dim(segment_adapter_index.reshape(ny), yi, 0, keepdims=False)
    coef_row = coefficient_row(adapter, adapter_rank_blocks, packed, padded)
    coef = lax.all_gather(
        jnp.broadcast_to(coef_row, (tokens, padded)), "x", axis=0, tiled=True
    )

    count = nx * tokens
    chunk = value_cols // layers
    sizes = (value_cols, chunk, packed, width)
    wire = value_cols + chunk + padded
    each = value_cols // (nz * nx * nc)
    steps = depth // STEP
    shape = jax.ShapeDtypeStruct
    call = functools.partial(
        pl.pallas_call,
        grid=(steps,),
        interpret=INTERPRET,
        compiler_params=pltpu.CompilerParams(vmem_limit_bytes=KERNEL_BYTES),
    )
    sent_shape, wide_shape = shape((count, wire), BF), shape((count, depth), BF)
    sums = [
        pltpu.VMEM((count, value_cols), F32),
        pltpu.VMEM((count, padded), F32),
        pltpu.VMEM((count, LANES), F32),
    ]
    top = layers - 1

    sent, last, scaled_input = call(
        functools.partial(forward_kernel, layer=0, sizes=sizes),
        out_shape=(sent_shape, shape((count, value_cols), BF), wide_shape),
        in_specs=[
            columns(count),
            weight(top, 1, value_cols),
            columns(count),
            weight(0, 0, value_cols),
            along(0, padded),
            along(0, 1),
        ],
        out_specs=(whole(), whole(), columns(count)),
        scratch_shapes=sums + [pltpu.VMEM((count, value_cols), F32)],
    )(grad, full, state, full, downs_full, gains)
    arrived, inputs, scaled = [gathered(sent)], [state], [scaled_input]
    for layer in range(1, layers):
        sent, state, scaled_input = call(
            functools.partial(forward_kernel, layer=layer, sizes=sizes),
            out_shape=(sent_shape, wide_shape, wide_shape),
            in_specs=[
                whole(),
                whole(),
                whole(),
                columns(count),
                weight(layer - 1, 1, value_cols),
                weight(layer, 0, value_cols),
                along(layer, padded),
                along(layer, 1),
                whole(),
            ],
            out_specs=(whole(), columns(count), columns(count)),
            scratch_shapes=sums + [pltpu.VMEM((count, value_cols), BF)],
        )(arrived[-1], coef, ups, state, full, full, downs_full, gains, last)
        arrived.append(gathered(sent))
        inputs.append(state)
        scaled.append(scaled_input)

    spots = (nz, nx, nc, each)
    place_ids = jnp.stack([xi, ci]).astype(jnp.int32)
    block_rows = packed + each * (padded // LANES)
    block_shape = (nz, block_rows, LANES)
    kept, crossed = [None] * layers, [None] * layers
    pieces = arrived
    for layer in reversed(range(layers)):
        bottom = layer == 0
        operands = [place_ids, *pieces, arrived[layer], coef, ups, scaled[layer]]
        specs = [
            pl.BlockSpec(memory_space=pltpu.SMEM),
            *[whole() for _ in pieces],
            whole(),
            whole(),
            whole(),
            columns(count),
        ]
        outs = [shape(block_shape, BF)] * 2
        out_specs = [whole()] * 2
        scratch = [pltpu.VMEM((count, padded), BF), pltpu.VMEM((value_cols, padded), F32)]
        if not bottom:
            operands += [inputs[layer], grad, full, downs_full, gains, full]
            specs += [
                columns(count),
                columns(count),
                weight(layer, 0, value_cols),
                along(layer, padded),
                along(layer, 1),
                weight(layer - 1, 1, value_cols),
            ]
            outs += [shape((count, value_cols), BF), wide_shape]
            out_specs += [whole(), columns(count)]
            scratch += [
                pltpu.VMEM((count, value_cols), BF),
                pltpu.VMEM((count, LANES), F32),
                pltpu.VMEM((count, value_cols), F32),
            ]
        results = call(
            functools.partial(
                backward_kernel, layer=layer, last=layer == top, sizes=sizes, spots=spots
            ),
            out_shape=outs,
            in_specs=specs,
            out_specs=out_specs,
            scratch_shapes=scratch,
        )(*operands)
        kept[layer] = results[0]
        crossed[layer] = lax.ppermute(results[1], "c", [(j, 1 - j) for j in range(nc)])
        if not bottom:
            grad = results[3]
            pieces = [gathered(results[2])]

    total = (jnp.stack(kept).astype(F32) + jnp.stack(crossed).astype(F32)).astype(BF)
    total = summed(exchanged(total, "y")).astype(BF)
    total = summed(exchanged(total, "z"))
    up = jnp.concatenate(
        [total[packed + k * each : packed + (k + 1) * each] for k in range(padded // LANES)],
        axis=1,
    )[:, :packed]
    return (total[:packed].T[None], up.T[None])


def solution(mesh):
    shape = mesh.devices.shape
    cores, across = 2, 4
    split = Mesh(
        mesh.devices.reshape(shape[0], shape[1] // (across * cores), across, cores),
        ("y", "z", "x", "c"),
    )
    fsdp = ("z", "x", "c")
    placed = (
        P(None, fsdp, None),
        P(None, fsdp, None),
        P("y", fsdp, None),
        P("y", None, fsdp),
        P("y", None, None),
        P("y", None, None),
        P("y", None),
        P(None, fsdp),
        P(),
    )
    return jax.shard_map(
        local,
        mesh=split,
        in_specs=placed,
        out_specs=(P("y", fsdp, None), P("y", None, fsdp)),
        check_vma=False,
    )
```

```python
import functools

import jax
import jax.numpy as jnp
from jax import lax
from jax.experimental import pallas as pl
from jax.experimental.layout import Layout, with_layout_constraint
from jax.experimental.pallas import tpu as pltpu
from jax.sharding import Mesh, PartitionSpec as P

ADAPTERS = 4
EPSILON = 1e-06
ADAPTER_ALPHA = 32.0
BF = jnp.bfloat16
F32 = jnp.float32
GROUP = ("y", "z", "c")
LANES = 128
STEP = 1024
INTERPRET = False
KERNEL_BYTES = 50 * 1024 * 1024


def contract(left, right, left_dim, right_dim):
    return lax.dot_general(
        left, right, (((left_dim,), (right_dim,)), ((), ())), preferred_element_type=F32
    )


def coefficient_row(adapter, adapter_rank_blocks, packed, columns):
    rank_sizes = 8 * adapter_rank_blocks
    adapters = jnp.arange(ADAPTERS, dtype=jnp.int32)
    ends = jnp.sum(
        jnp.where(adapters[None, :] <= adapters[:, None], rank_sizes[None, :], 0), axis=1
    )
    column = jnp.arange(columns, dtype=jnp.int32)
    owner = jnp.sum((column[:, None] >= ends[None, :]).astype(jnp.int32), axis=1)
    rank = jnp.sum(jnp.where(adapters == adapter, rank_sizes, 0)).astype(F32)
    held = (owner == adapter) & (column < packed)
    return jnp.where(held, ADAPTER_ALPHA / rank, 0.0)[None, :]


def exchanged(value, axis):
    return lax.all_to_all(value, axis, split_axis=0, concat_axis=0, tiled=True)


def summed(value):
    return value.astype(F32).sum(axis=0)


def gathered(partial):
    return lax.all_gather(partial, "x", axis=0, tiled=False)


def token_stats(gathered_ref, value_cols, chunk, packed, width):
    total = gathered_ref[...].astype(F32).sum(axis=0)
    side = total[:, value_cols + chunk :]
    mean = (side[:, packed : packed + 1] + side[:, packed + 1 : packed + 2]) / width
    return total[:, :value_cols], side, lax.rsqrt(mean + EPSILON)


def forward_kernel(*refs, layer, sizes):
    value_cols, chunk, packed, width = sizes
    first = layer == 0
    if first:
        grad, last_out, state, value_w, down_w, gain, sent, last_sum, scaled = refs[:9]
        acc, side_acc, square_acc, last_acc = refs[9:]
    else:
        before, coef, up, state, out_w, value_w, down_w, gain, last_piece = refs[:9]
        sent, new_state, scaled = refs[9:12]
        acc, side_acc, square_acc, values = refs[12:]
    step = pl.program_id(0)

    @pl.when(step == 0)
    def _():
        acc[...] = jnp.zeros_like(acc)
        side_acc[...] = jnp.zeros_like(side_acc)
        square_acc[...] = jnp.zeros_like(square_acc)
        if first:
            last_acc[...] = jnp.zeros_like(last_acc)
        else:
            value_part, side, inv = token_stats(before, value_cols, chunk, packed, width)
            low = (side * inv * coef[...]).astype(BF)
            values[...] = (value_part * inv + contract(low, up[layer - 1], 1, 0)).astype(BF)

    if first:
        wide = state[...].astype(F32)
        last_acc[...] += contract(grad[...], last_out[0], 1, 0)
    else:
        wide = state[...].astype(F32) + contract(values[...], out_w[0], 1, 1)
        new_state[...] = wide.astype(BF)
        wide = new_state[...].astype(F32)
    square_acc[...] += jnp.sum(wide * wide, axis=1, keepdims=True)
    scaled_input = (wide * gain[0]).astype(BF)
    scaled[...] = scaled_input
    acc[...] += contract(scaled_input, value_w[0], 1, 0)
    side_acc[...] += contract(scaled_input, down_w[0], 1, 1)

    @pl.when(step == pl.num_programs(0) - 1)
    def _():
        sent[:, :value_cols] = acc[...].astype(BF)
        if first:
            last = last_acc[...].astype(BF)
            last_sum[...] = last
            sent[:, value_cols : value_cols + chunk] = last[:, :chunk]
        else:
            sent[:, value_cols : value_cols + chunk] = last_piece[
                :, layer * chunk : (layer + 1) * chunk
            ]
        squares = square_acc[:, :1]
        high = squares.astype(BF).astype(F32)
        lane = lax.broadcasted_iota(jnp.int32, side_acc.shape, 1)
        side = jnp.where(lane == packed, high, side_acc[...])
        side = jnp.where(lane == packed + 1, squares - high, side)
        sent[:, value_cols + chunk :] = side.astype(BF)


def backward_kernel(*refs, layer, last, sizes, spots):
    value_cols, chunk, packed, width = sizes
    bottom = layer == 0
    nz, nx, nc, each = spots
    refs = list(refs)
    take = lambda n: [refs.pop(0) for _ in range(n)]
    where, = take(1)
    pieces = take(value_cols // chunk if last else 1)
    before, coef, up, scaled = take(4)
    if not bottom:
        state, grad, value_w, down_w, gain, out_w = take(6)
    own, other = take(2)
    if not bottom:
        sent, new_grad = take(2)
    mixed_low, raised = take(2)
    if not bottom:
        mixed_value, kappa, acc = take(3)
    step = pl.program_id(0)
    xi, ci = where[0], where[1]

    @pl.when(step == 0)
    def _():
        first = value_cols if last else 0
        wide = chunk if last else value_cols
        summed_pieces = [
            piece[:, :, first : first + wide].astype(F32).sum(axis=0) for piece in pieces
        ]
        total = summed_pieces[0] if len(pieces) == 1 else jnp.concatenate(summed_pieces, axis=1)
        value_grad = total.astype(BF)
        wide_value = value_grad.astype(F32)
        low_grad = (contract(value_grad, up[layer], 1, 1) * coef[...]).astype(BF)
        wide_low = low_grad.astype(F32)
        value_part, side, inv = token_stats(before, value_cols, chunk, packed, width)
        mixed_low[...] = (wide_low * inv).astype(BF)
        if not bottom:
            mixed_value[...] = (wide_value * inv).astype(BF)
            inner = jnp.sum(value_part * wide_value, axis=1, keepdims=True)
            inner = inner + jnp.sum(side * wide_low, axis=1, keepdims=True)
            kappa[...] = jnp.broadcast_to(inv * inv * inv * inner / width, kappa.shape)
            acc[...] = jnp.zeros_like(acc)
        low = (side * inv * coef[...]).astype(BF)
        raised[...] = contract(value_grad, low, 0, 0)
        for z in range(nz):
            for target, core in ((own, ci), (other, 1 - ci)):
                row = pl.multiple_of((z * nx + xi) * nc * each + core * each, each)
                piece = raised[pl.ds(row, each), :]
                target[z, packed:, :] = jnp.concatenate(
                    [piece[:, k * LANES : (k + 1) * LANES] for k in range(piece.shape[1] // LANES)],
                    axis=0,
                ).astype(BF)

    lowered = contract(mixed_low[...], scaled[...], 0, 0)[:packed]
    per_step = scaled.shape[1] // (nc * LANES)
    for k in range(per_step):
        start = k * nc * LANES
        one = lowered[:, start : start + LANES]
        two = lowered[:, start + LANES : start + 2 * LANES]
        own[step * per_step + k, :packed, :] = jnp.where(ci == 0, one, two).astype(BF)
        other[step * per_step + k, :packed, :] = jnp.where(ci == 0, two, one).astype(BF)
    if not bottom:
        back = contract(mixed_value[...], value_w[0], 1, 1)
        back = back + contract(mixed_low[...], down_w[0], 1, 0)
        wide = grad[...].astype(F32) + gain[0] * back - kappa[:, :1] * state[...].astype(F32)
        updated = wide.astype(BF)
        new_grad[...] = updated
        acc[...] += contract(updated, out_w[0], 1, 0)

        @pl.when(step == pl.num_programs(0) - 1)
        def _():
            sent[...] = acc[...].astype(BF)


def whole():
    return pl.BlockSpec(memory_space=pltpu.VMEM)


def columns(tokens):
    return pl.BlockSpec((tokens, STEP), lambda i: (0, i))


def weight(layer, half, cols):
    return pl.BlockSpec((1, STEP, cols), lambda i: (layer, i, half))


def along(layer, rows):
    return pl.BlockSpec((1, rows, STEP), lambda i: (layer, 0, i))


def local(
    residual_input,
    output_gradient,
    value_projection_weight,
    output_weight,
    adapter_down_weight,
    adapter_up_weight,
    input_norm_scale,
    segment_adapter_index,
    adapter_rank_blocks,
):
    ny, nz, nx, nc = (lax.axis_size(name) for name in ("y", "z", "x", "c"))
    yi, zi, xi, ci = (lax.axis_index(name) for name in ("y", "z", "x", "c"))
    rows = value_projection_weight.shape[1]
    value_cols = value_projection_weight.shape[2]
    packed = adapter_down_weight.shape[2]
    width = adapter_down_weight.shape[1]
    both = value_cols + packed
    layers = ny
    lanes = nc * rows
    depth = nz * lanes

    joined = jnp.concatenate([value_projection_weight[0], output_weight[0].T], axis=1)
    joined = with_layout_constraint(joined, Layout(major_to_minor=(0, 1)))
    full = lax.all_gather(joined, GROUP, axis=0, tiled=False)
    full = with_layout_constraint(full, Layout(major_to_minor=(0, 1, 2)))
    full = full.reshape(layers, depth, 2 * value_cols)

    all_tokens = residual_input.shape[0] * residual_input.shape[1]
    tokens = all_tokens // ny
    first = yi * tokens
    own = jnp.stack(
        [
            lax.dynamic_slice(array.reshape(all_tokens, width), (first, 0), (tokens, width))
            for array in (residual_input, output_gradient)
        ]
    )
    own = own.reshape(2, tokens, nz, nx, lanes).transpose(3, 0, 1, 2, 4)
    spread = exchanged(own.reshape(nx, 2, tokens, depth), "x")
    state = spread[:, 0].reshape(nx * tokens, depth)
    grad = spread[:, 1].reshape(nx * tokens, depth)

    padded = -(-packed // LANES) * LANES
    half = packed // nc
    down_half = lax.dynamic_slice(
        adapter_down_weight[0].T.reshape(packed, nz, nx, lanes),
        (ci * half, 0, xi, 0),
        (half, nz, 1, lanes),
    ).reshape(1, half, depth)
    mine = exchanged(jnp.broadcast_to(down_half, (layers, half, depth)), "y")
    theirs = lax.ppermute(mine, "c", [(j, 1 - j) for j in range(nc)])
    ordered = [jnp.where(ci == 0, mine, theirs), jnp.where(ci == 0, theirs, mine)]
    filler = jnp.zeros((layers, padded - packed, depth), BF)
    downs_full = jnp.concatenate(ordered + [filler], axis=1)

    gain_own = lax.dynamic_index_in_dim(
        input_norm_scale.reshape(nz, nx, lanes), xi, 1, keepdims=False
    ).reshape(depth // value_cols, value_cols)
    high = lax.reduce_precision(gain_own, 8, 7)
    middle = lax.reduce_precision(gain_own - high, 8, 7)
    parts = [high, middle, gain_own - high - middle]
    small = jnp.concatenate([adapter_up_weight[0]] + [part.astype(BF) for part in parts], axis=0)
    small = lax.all_gather(small, "y", axis=0, tiled=False)
    ups = jnp.pad(small[:, :packed], ((0, 0), (0, padded - packed), (0, 0)))
    gains = small[:, packed:].astype(F32).reshape(layers, 3, 1, depth)
    gains = gains[:, 0] + gains[:, 1] + gains[:, 2]
    adapter = lax.dynamic_index_in_dim(segment_adapter_index.reshape(ny), yi, 0, keepdims=False)
    coef_row = coefficient_row(adapter, adapter_rank_blocks, packed, padded)
    coef = lax.all_gather(
        jnp.broadcast_to(coef_row, (tokens, padded)), "x", axis=0, tiled=True
    )

    count = nx * tokens
    chunk = value_cols // layers
    sizes = (value_cols, chunk, packed, width)
    wire = value_cols + chunk + padded
    each = value_cols // (nz * nx * nc)
    steps = depth // STEP
    shape = jax.ShapeDtypeStruct
    call = functools.partial(
        pl.pallas_call,
        grid=(steps,),
        interpret=INTERPRET,
        compiler_params=pltpu.CompilerParams(vmem_limit_bytes=KERNEL_BYTES),
    )
    sent_shape, wide_shape = shape((count, wire), BF), shape((count, depth), BF)
    sums = [
        pltpu.VMEM((count, value_cols), F32),
        pltpu.VMEM((count, padded), F32),
        pltpu.VMEM((count, LANES), F32),
    ]
    top = layers - 1

    sent, last, scaled_input = call(
        functools.partial(forward_kernel, layer=0, sizes=sizes),
        out_shape=(sent_shape, shape((count, value_cols), BF), wide_shape),
        in_specs=[
            columns(count),
            weight(top, 1, value_cols),
            columns(count),
            weight(0, 0, value_cols),
            along(0, padded),
            along(0, 1),
        ],
        out_specs=(whole(), whole(), columns(count)),
        scratch_shapes=sums + [pltpu.VMEM((count, value_cols), F32)],
    )(grad, full, state, full, downs_full, gains)
    arrived, inputs, scaled = [gathered(sent)], [state], [scaled_input]
    for layer in range(1, layers):
        sent, state, scaled_input = call(
            functools.partial(forward_kernel, layer=layer, sizes=sizes),
            out_shape=(sent_shape, wide_shape, wide_shape),
            in_specs=[
                whole(),
                whole(),
                whole(),
                columns(count),
                weight(layer - 1, 1, value_cols),
                weight(layer, 0, value_cols),
                along(layer, padded),
                along(layer, 1),
                whole(),
            ],
            out_specs=(whole(), columns(count), columns(count)),
            scratch_shapes=sums + [pltpu.VMEM((count, value_cols), BF)],
        )(arrived[-1], coef, ups, state, full, full, downs_full, gains, last)
        arrived.append(gathered(sent))
        inputs.append(state)
        scaled.append(scaled_input)

    spots = (nz, nx, nc, each)
    place_ids = jnp.stack([xi, ci]).astype(jnp.int32)
    block_rows = packed + each * (padded // LANES)
    block_shape = (nz, block_rows, LANES)
    kept, crossed = [None] * layers, [None] * layers
    pieces = arrived
    for layer in reversed(range(layers)):
        bottom = layer == 0
        operands = [place_ids, *pieces, arrived[layer], coef, ups, scaled[layer]]
        specs = [
            pl.BlockSpec(memory_space=pltpu.SMEM),
            *[whole() for _ in pieces],
            whole(),
            whole(),
            whole(),
            columns(count),
        ]
        outs = [shape(block_shape, BF)] * 2
        out_specs = [whole()] * 2
        scratch = [pltpu.VMEM((count, padded), BF), pltpu.VMEM((value_cols, padded), F32)]
        if not bottom:
            operands += [inputs[layer], grad, full, downs_full, gains, full]
            specs += [
                columns(count),
                columns(count),
                weight(layer, 0, value_cols),
                along(layer, padded),
                along(layer, 1),
                weight(layer - 1, 1, value_cols),
            ]
            outs += [shape((count, value_cols), BF), wide_shape]
            out_specs += [whole(), columns(count)]
            scratch += [
                pltpu.VMEM((count, value_cols), BF),
                pltpu.VMEM((count, LANES), F32),
                pltpu.VMEM((count, value_cols), F32),
            ]
        results = call(
            functools.partial(
                backward_kernel, layer=layer, last=layer == top, sizes=sizes, spots=spots
            ),
            out_shape=outs,
            in_specs=specs,
            out_specs=out_specs,
            scratch_shapes=scratch,
        )(*operands)
        kept[layer] = results[0]
        crossed[layer] = lax.ppermute(results[1], "c", [(j, 1 - j) for j in range(nc)])
        if not bottom:
            grad = results[3]
            pieces = [gathered(results[2])]

    total = (jnp.stack(kept).astype(F32) + jnp.stack(crossed).astype(F32)).astype(BF)
    total = summed(exchanged(total, "y")).astype(BF)
    total = summed(exchanged(total, "z"))
    up = jnp.concatenate(
        [total[packed + k * each : packed + (k + 1) * each] for k in range(padded // LANES)],
        axis=1,
    )[:, :packed]
    return (total[:packed].T[None], up.T[None])


def solution(mesh):
    shape = mesh.devices.shape
    cores, across = 2, 4
    split = Mesh(
        mesh.devices.reshape(shape[0], shape[1] // (across * cores), across, cores),
        ("y", "z", "x", "c"),
    )
    fsdp = ("z", "x", "c")
    placed = (
        P(None, fsdp, None),
        P(None, fsdp, None),
        P("y", fsdp, None),
        P("y", None, fsdp),
        P("y", None, None),
        P("y", None, None),
        P("y", None),
        P(None, fsdp),
        P(),
    )
    return jax.shard_map(
        local,
        mesh=split,
        in_specs=placed,
        out_specs=(P("y", fsdp, None), P("y", None, fsdp)),
        check_vma=False,
    )
```

```python
import functools

import jax
import jax.numpy as jnp
from jax import lax
from jax.experimental import pallas as pl
from jax.experimental.layout import Layout, with_layout_constraint
from jax.experimental.pallas import tpu as pltpu
from jax.sharding import Mesh, PartitionSpec as P

ADAPTERS = 4
EPSILON = 1e-06
ADAPTER_ALPHA = 32.0
BF = jnp.bfloat16
F32 = jnp.float32
GROUP = ("y", "z", "c")
LANES = 128
STEP = 1024
INTERPRET = False
REST = 128
KERNEL_BYTES = 50 * 1024 * 1024


def contract(left, right, left_dim, right_dim):
    return lax.dot_general(
        left, right, (((left_dim,), (right_dim,)), ((), ())), preferred_element_type=F32
    )


def coefficient_table(adapter_rank_blocks, packed, columns):
    rank_sizes = 8 * adapter_rank_blocks
    adapters = jnp.arange(ADAPTERS, dtype=jnp.int32)
    ends = jnp.sum(
        jnp.where(adapters[None, :] <= adapters[:, None], rank_sizes[None, :], 0), axis=1
    )
    column = jnp.arange(columns, dtype=jnp.int32)
    owner = jnp.sum((column[:, None] >= ends[None, :]).astype(jnp.int32), axis=1)
    owner = jnp.where(column < packed, owner, -1)
    rank = jnp.sum(
        jnp.where(owner[:, None] == adapters[None, :], rank_sizes[None, :], 0), axis=1
    ).astype(F32)
    value = jnp.where(owner >= 0, ADAPTER_ALPHA / jnp.maximum(rank, 1.0), 0.0)
    spare = jnp.zeros((6, columns), F32)
    return jnp.concatenate([owner.astype(F32)[None], value[None], spare], axis=0)


def exchanged(value, axis):
    return lax.all_to_all(value, axis, split_axis=0, concat_axis=0, tiled=True)


def summed(value):
    return value.astype(F32).sum(axis=0)


def gathered(partial):
    return lax.all_gather(partial, "x", axis=0, tiled=False)


def token_stats(gathered_ref, table, value_cols, chunk, packed, width):
    total = gathered_ref[...].astype(F32).sum(axis=0)
    side = total[:, value_cols + chunk :]
    mean = (side[:, packed : packed + 1] + side[:, packed + 1 : packed + 2]) / width
    adapter = side[:, packed + 2 : packed + 3]
    coef = jnp.where(table[:1, :] == adapter, table[1:2, :], 0.0)
    return total[:, :value_cols], side, lax.rsqrt(mean + EPSILON), coef


def forward_kernel(*refs, layer, sizes):
    value_cols, chunk, packed, width = sizes
    first = layer == 0
    if first:
        own_ids, grad, last_out, last_rest, state, value_w, down_w, gain = refs[:8]
        sent, last_sum, scaled, acc, side_acc, square_acc, last_acc = refs[8:]
    else:
        own_ids, before, table, up, state, out_w, rest_w, value_w, down_w, gain = refs[:10]
        last_piece, sent, new_state, scaled = refs[10:14]
        acc, side_acc, square_acc, values = refs[14:]
    step = pl.program_id(0)

    @pl.when(step == 0)
    def _():
        acc[...] = jnp.zeros_like(acc)
        side_acc[...] = jnp.zeros_like(side_acc)
        square_acc[...] = jnp.zeros_like(square_acc)
        if first:
            last_acc[...] = jnp.zeros_like(last_acc)
        else:
            value_part, side, inv, coef = token_stats(
                before, table, value_cols, chunk, packed, width
            )
            low = (side * inv * coef).astype(BF)
            values[...] = (value_part * inv + contract(low, up[layer - 1], 1, 0)).astype(BF)

    if first:
        wide = state[...].astype(F32)
        most = last_out.shape[2]
        last_acc[:, :most] += contract(grad[...], last_out[0], 1, 0)
        last_acc[:, most:] += contract(grad[...], last_rest[0], 1, 1)
    else:
        most = out_w.shape[2]
        wide = state[...].astype(F32) + contract(values[:, :most], out_w[0], 1, 1)
        wide = wide + contract(values[:, most:], rest_w[0], 1, 0)
        new_state[...] = wide.astype(BF)
        wide = new_state[...].astype(F32)
    square_acc[...] += jnp.sum(wide * wide, axis=1, keepdims=True)
    scaled_input = (wide * gain[0]).astype(BF)
    scaled[...] = scaled_input
    acc[...] += contract(scaled_input, value_w[0], 1, 0)
    side_acc[...] += contract(scaled_input, down_w[0], 1, 1)

    @pl.when(step == pl.num_programs(0) - 1)
    def _():
        sent[:, :value_cols] = acc[...].astype(BF)
        if first:
            last = last_acc[...].astype(BF)
            last_sum[...] = last
            sent[:, value_cols : value_cols + chunk] = last[:, :chunk]
        else:
            sent[:, value_cols : value_cols + chunk] = last_piece[
                :, layer * chunk : (layer + 1) * chunk
            ]
        squares = square_acc[:, :1]
        high = squares.astype(BF).astype(F32)
        lane = lax.broadcasted_iota(jnp.int32, side_acc.shape, 1)
        side = jnp.where(lane == packed, high, side_acc[...])
        side = jnp.where(lane == packed + 1, squares - high, side)
        side = jnp.where(lane == packed + 2, own_ids[:, :1], side)
        sent[:, value_cols + chunk :] = side.astype(BF)


def backward_kernel(*refs, layer, last, sizes, spots):
    value_cols, chunk, packed, width = sizes
    bottom = layer == 0
    nz, nx, nc, each = spots
    refs = list(refs)
    take = lambda n: [refs.pop(0) for _ in range(n)]
    where, = take(1)
    pieces = take(value_cols // chunk if last else 1)
    before, table, up, scaled = take(4)
    if not bottom:
        state, grad, value_w, down_w, gain, out_w, rest_w = take(7)
    own, other = take(2)
    if not bottom:
        sent, new_grad = take(2)
    mixed_low, raised = take(2)
    if not bottom:
        mixed_value, kappa, acc = take(3)
    step = pl.program_id(0)
    xi, ci = where[0], where[1]

    @pl.when(step == 0)
    def _():
        first = value_cols if last else 0
        wide = chunk if last else value_cols
        summed_pieces = [
            piece[:, :, first : first + wide].astype(F32).sum(axis=0) for piece in pieces
        ]
        total = summed_pieces[0] if len(pieces) == 1 else jnp.concatenate(summed_pieces, axis=1)
        value_grad = total.astype(BF)
        wide_value = value_grad.astype(F32)
        value_part, side, inv, coef = token_stats(
            before, table, value_cols, chunk, packed, width
        )
        low_grad = (contract(value_grad, up[layer], 1, 1) * coef).astype(BF)
        wide_low = low_grad.astype(F32)
        mixed_low[...] = (wide_low * inv).astype(BF)
        if not bottom:
            mixed_value[...] = (wide_value * inv).astype(BF)
            inner = jnp.sum(value_part * wide_value, axis=1, keepdims=True)
            inner = inner + jnp.sum(side * wide_low, axis=1, keepdims=True)
            kappa[...] = jnp.broadcast_to(inv * inv * inv * inner / width, kappa.shape)
            acc[...] = jnp.zeros_like(acc)
        low = (side * inv * coef).astype(BF)
        raised[...] = contract(value_grad, low, 0, 0)
        for z in range(nz):
            for target, core in ((own, ci), (other, 1 - ci)):
                row = pl.multiple_of((z * nx + xi) * nc * each + core * each, each)
                piece = raised[pl.ds(row, each), :]
                target[z, packed:, :] = jnp.concatenate(
                    [piece[:, k * LANES : (k + 1) * LANES] for k in range(piece.shape[1] // LANES)],
                    axis=0,
                ).astype(BF)

    lowered = contract(mixed_low[...], scaled[...], 0, 0)[:packed]
    per_step = scaled.shape[1] // (nc * LANES)
    for k in range(per_step):
        start = k * nc * LANES
        one = lowered[:, start : start + LANES]
        two = lowered[:, start + LANES : start + 2 * LANES]
        own[step * per_step + k, :packed, :] = jnp.where(ci == 0, one, two).astype(BF)
        other[step * per_step + k, :packed, :] = jnp.where(ci == 0, two, one).astype(BF)
    if not bottom:
        back = contract(mixed_value[...], value_w[0], 1, 1)
        back = back + contract(mixed_low[...], down_w[0], 1, 0)
        wide = grad[...].astype(F32) + gain[0] * back - kappa[:, :1] * state[...].astype(F32)
        updated = wide.astype(BF)
        new_grad[...] = updated
        most = out_w.shape[2]
        acc[:, :most] += contract(updated, out_w[0], 1, 0)
        acc[:, most:] += contract(updated, rest_w[0], 1, 1)

        @pl.when(step == pl.num_programs(0) - 1)
        def _():
            sent[...] = acc[...].astype(BF)


def whole():
    return pl.BlockSpec(memory_space=pltpu.VMEM)


def columns(tokens):
    return pl.BlockSpec((tokens, STEP), lambda i: (0, i))


def value_part_of(layer, cols):
    return pl.BlockSpec((1, STEP, cols), lambda i: (layer, i, 0))


def out_parts_of(layer, cols):
    return [
        pl.BlockSpec(
            (pl.Element(1), pl.Element(STEP), pl.Element(cols - REST)),
            lambda i: (layer, i * STEP, cols),
        ),
        pl.BlockSpec((1, REST, STEP), lambda i: (layer, 0, i)),
    ]


def along(layer, rows):
    return pl.BlockSpec((1, rows, STEP), lambda i: (layer, 0, i))


def local(
    residual_input,
    output_gradient,
    value_projection_weight,
    output_weight,
    adapter_down_weight,
    adapter_up_weight,
    input_norm_scale,
    segment_adapter_index,
    adapter_rank_blocks,
):
    ny, nz, nx, nc = (lax.axis_size(name) for name in ("y", "z", "x", "c"))
    yi, zi, xi, ci = (lax.axis_index(name) for name in ("y", "z", "x", "c"))
    rows = value_projection_weight.shape[1]
    value_cols = value_projection_weight.shape[2]
    packed = adapter_down_weight.shape[2]
    width = adapter_down_weight.shape[1]
    both = value_cols + packed
    layers = ny
    lanes = nc * rows
    depth = nz * lanes

    most = value_cols - REST
    joined = jnp.concatenate([value_projection_weight[0], output_weight[0, :most].T], axis=1)
    joined = with_layout_constraint(joined, Layout(major_to_minor=(0, 1)))
    full = lax.all_gather(joined, GROUP, axis=0, tiled=False)
    full = with_layout_constraint(full, Layout(major_to_minor=(0, 1, 2)))
    full = full.reshape(layers, depth, value_cols + most)
    rest = lax.all_gather(output_weight[0, most:], "z", axis=0, tiled=False)

    all_tokens = residual_input.shape[0] * residual_input.shape[1]
    tokens = all_tokens // ny
    first = yi * tokens
    own = jnp.stack(
        [
            lax.dynamic_slice(array.reshape(all_tokens, width), (first, 0), (tokens, width))
            for array in (residual_input, output_gradient)
        ]
    )
    own = own.reshape(2, tokens, nz, nx, lanes).transpose(3, 0, 1, 2, 4)
    spread = exchanged(own.reshape(nx, 2, tokens, depth), "x")
    state = spread[:, 0].reshape(nx * tokens, depth)
    grad = spread[:, 1].reshape(nx * tokens, depth)

    padded = -(-packed // LANES) * LANES
    down_half = lax.dynamic_slice(
        adapter_down_weight[0].T.reshape(packed, nz, nx, nc, rows),
        (0, 0, xi, ci, 0),
        (packed, nz, 1, 1, rows),
    ).reshape(packed, nz * rows)
    rest = rest.transpose(1, 0, 2).reshape(REST, nz * rows)
    beside = jnp.concatenate([down_half, rest], axis=0)
    mine = exchanged(jnp.broadcast_to(beside[None], (layers,) + beside.shape), "y")
    theirs = lax.ppermute(mine, "c", [(j, 1 - j) for j in range(nc)])
    ordered = [jnp.where(ci == 0, mine, theirs), jnp.where(ci == 0, theirs, mine)]
    pieces = [part[..., z * rows : (z + 1) * rows] for z in range(nz) for part in ordered]
    downs_full = jnp.concatenate([piece[:, :packed] for piece in pieces], axis=2)
    downs_full = jnp.pad(downs_full, ((0, 0), (0, padded - packed), (0, 0)))
    rest_full = jnp.concatenate([piece[:, packed:] for piece in pieces], axis=2)

    gain_own = lax.dynamic_index_in_dim(
        input_norm_scale.reshape(nz, nx, lanes), xi, 1, keepdims=False
    ).reshape(depth // value_cols, value_cols)
    high = lax.reduce_precision(gain_own, 8, 7)
    middle = lax.reduce_precision(gain_own - high, 8, 7)
    parts = [high, middle, gain_own - high - middle]
    small = jnp.concatenate([adapter_up_weight[0]] + [part.astype(BF) for part in parts], axis=0)
    small = lax.all_gather(small, "y", axis=0, tiled=False)
    ups = jnp.pad(small[:, :packed], ((0, 0), (0, padded - packed), (0, 0)))
    gains = small[:, packed:].astype(F32).reshape(layers, 3, 1, depth)
    gains = gains[:, 0] + gains[:, 1] + gains[:, 2]
    adapter = lax.dynamic_index_in_dim(segment_adapter_index.reshape(ny), yi, 0, keepdims=False)
    table = coefficient_table(adapter_rank_blocks, packed, padded)
    holder = jnp.arange(nx * tokens, dtype=jnp.int32)[:, None] // tokens
    own_ids = jnp.where(holder == xi, adapter.astype(F32), 0.0)
    own_ids = jnp.broadcast_to(own_ids, (nx * tokens, LANES))

    count = nx * tokens
    chunk = value_cols // layers
    sizes = (value_cols, chunk, packed, width)
    wire = value_cols + chunk + padded
    each = value_cols // (nz * nx * nc)
    steps = depth // STEP
    shape = jax.ShapeDtypeStruct
    call = functools.partial(
        pl.pallas_call,
        grid=(steps,),
        interpret=INTERPRET,
        compiler_params=pltpu.CompilerParams(vmem_limit_bytes=KERNEL_BYTES),
    )
    sent_shape, wide_shape = shape((count, wire), BF), shape((count, depth), BF)
    sums = [
        pltpu.VMEM((count, value_cols), F32),
        pltpu.VMEM((count, padded), F32),
        pltpu.VMEM((count, LANES), F32),
    ]
    top = layers - 1

    sent, last, scaled_input = call(
        functools.partial(forward_kernel, layer=0, sizes=sizes),
        out_shape=(sent_shape, shape((count, value_cols), BF), wide_shape),
        in_specs=[
            whole(),
            columns(count),
            *out_parts_of(top, value_cols),
            columns(count),
            value_part_of(0, value_cols),
            along(0, padded),
            along(0, 1),
        ],
        out_specs=(whole(), whole(), columns(count)),
        scratch_shapes=sums + [pltpu.VMEM((count, value_cols), F32)],
    )(own_ids, grad, full, rest_full, state, full, downs_full, gains)
    arrived, inputs, scaled = [gathered(sent)], [state], [scaled_input]
    for layer in range(1, layers):
        sent, state, scaled_input = call(
            functools.partial(forward_kernel, layer=layer, sizes=sizes),
            out_shape=(sent_shape, wide_shape, wide_shape),
            in_specs=[
                whole(),
                whole(),
                whole(),
                whole(),
                columns(count),
                *out_parts_of(layer - 1, value_cols),
                value_part_of(layer, value_cols),
                along(layer, padded),
                along(layer, 1),
                whole(),
            ],
            out_specs=(whole(), columns(count), columns(count)),
            scratch_shapes=sums + [pltpu.VMEM((count, value_cols), BF)],
        )(
            own_ids,
            arrived[-1],
            table,
            ups,
            state,
            full,
            rest_full,
            full,
            downs_full,
            gains,
            last,
        )
        arrived.append(gathered(sent))
        inputs.append(state)
        scaled.append(scaled_input)

    spots = (nz, nx, nc, each)
    place_ids = jnp.stack([xi, ci]).astype(jnp.int32)
    block_rows = packed + each * (padded // LANES)
    block_shape = (nz, block_rows, LANES)
    kept, crossed = [None] * layers, [None] * layers
    pieces = arrived
    for layer in reversed(range(layers)):
        bottom = layer == 0
        operands = [place_ids, *pieces, arrived[layer], table, ups, scaled[layer]]
        specs = [
            pl.BlockSpec(memory_space=pltpu.SMEM),
            *[whole() for _ in pieces],
            whole(),
            whole(),
            whole(),
            columns(count),
        ]
        outs = [shape(block_shape, BF)] * 2
        out_specs = [whole()] * 2
        scratch = [pltpu.VMEM((count, padded), BF), pltpu.VMEM((value_cols, padded), F32)]
        if not bottom:
            operands += [inputs[layer], grad, full, downs_full, gains, full, rest_full]
            specs += [
                columns(count),
                columns(count),
                value_part_of(layer, value_cols),
                along(layer, padded),
                along(layer, 1),
                *out_parts_of(layer - 1, value_cols),
            ]
            outs += [shape((count, value_cols), BF), wide_shape]
            out_specs += [whole(), columns(count)]
            scratch += [
                pltpu.VMEM((count, value_cols), BF),
                pltpu.VMEM((count, LANES), F32),
                pltpu.VMEM((count, value_cols), F32),
            ]
        results = call(
            functools.partial(
                backward_kernel, layer=layer, last=layer == top, sizes=sizes, spots=spots
            ),
            out_shape=outs,
            in_specs=specs,
            out_specs=out_specs,
            scratch_shapes=scratch,
        )(*operands)
        kept[layer] = results[0]
        crossed[layer] = lax.ppermute(results[1], "c", [(j, 1 - j) for j in range(nc)])
        if not bottom:
            grad = results[3]
            pieces = [gathered(results[2])]

    total = (jnp.stack(kept).astype(F32) + jnp.stack(crossed).astype(F32)).astype(BF)
    total = summed(exchanged(total, "y")).astype(BF)
    total = summed(exchanged(total, "z"))
    up = jnp.concatenate(
        [total[packed + k * each : packed + (k + 1) * each] for k in range(padded // LANES)],
        axis=1,
    )[:, :packed]
    return (total[:packed].T[None], up.T[None])


def solution(mesh):
    shape = mesh.devices.shape
    cores, across = 2, 4
    split = Mesh(
        mesh.devices.reshape(shape[0], shape[1] // (across * cores), across, cores),
        ("y", "z", "x", "c"),
    )
    fsdp = ("z", "x", "c")
    placed = (
        P(None, fsdp, None),
        P(None, fsdp, None),
        P("y", fsdp, None),
        P("y", None, fsdp),
        P("y", None, None),
        P("y", None, None),
        P("y", None),
        P(None, fsdp),
        P(),
    )
    return jax.shard_map(
        local,
        mesh=split,
        in_specs=placed,
        out_specs=(P("y", fsdp, None), P("y", None, fsdp)),
        check_vma=False,
    )
```
